32 devices in a mesh: section: 2 (over y), dp: 4 (over x, core), mp: 4 (over z).
Axes of the slice: x: 2, y: 2, z: 4, core: 2. Of those that a mesh axis runs over, the one named last changes fastest.
Arguments:
- patches: bfloat16 [4096, 1280], P(('section', 'dp')), may hold values from -6 to 6
- patch_counts: int32 [16], P(('section', 'dp')), may hold values from 64 to 256, as said below
- dest_rows: int32 [1024], P(('section', 'dp')), may hold values from 0 to 4095, as said below
- qkv_weight: bfloat16 [1280, 3, 1280], P(None, None, 'mp'), may hold values from -1 to 1
- out_weight: bfloat16 [1280, 1280], P('mp'), may hold values from -0.15625 to 0.15625
- attn_gain: bfloat16 [1280], replicated, may hold values from 0.25 to 1.75
- merge_gain: bfloat16 [1280], replicated, may hold values from 0.25 to 1.75
- fc1_weight: bfloat16 [5120, 5120], P('mp', ('section', 'dp')), may hold values from -0.078125 to 0.078125
- fc1_bias: bfloat16 [5120], P(('section', 'dp')), may hold values from -3 to 3
- fc2_weight: bfloat16 [5120, 8192], P(('section', 'dp'), 'mp'), may hold values from -0.078125 to 0.078125
- fc2_bias: bfloat16 [8192], P('mp'), may hold values from -3 to 3
- text_embeds: bfloat16 [4096, 8192], P(('section', 'dp'), 'mp'), may hold values from -6 to 6
- section_hidden: bfloat16 [4096, 8192], P(('section', 'dp'), 'mp'), may hold values from -80 to 80
- llm_gain: bfloat16 [8192], P('mp'), may hold values from 0.25 to 1.75
Outputs:
- sequence_embeds: bfloat16 [4096, 8192], P(('section', 'dp'), 'mp')
- layer_inputs: bfloat16 [4096, 8192], P(('section', 'dp'), 'mp')
The draws below stay inside these ranges and needn't reach their ends.
Inputs may be any that keep to these rules, and one draw needn't show every extreme that they name: `patch_counts`: multiples of 4; a tile's patches fill the first slots of its block. `dest_rows`: all rows differ. Each group's merged slots form runs of 16 consecutive slots (aligned); a run goes to one sequence slice (row // 512, numbered in section-major order), different runs of a group to different slices. Rows of slots that are not live are never written.
All inputs are finite; a program needn't handle non-finite values.
Results may differ from the reference program's by a relative error of at most 0.0055.
Values may be sent and summed in bfloat16 or wider, within the bound.
A program may use at most 128 MiB of HBM per device.

```python
import math
import jax
import jax.numpy as jnp
from jax import lax

D_VIT = 1280
HEADS = 16
HEAD_DIM = 80
MERGE_HID = 5120
HID = 8192
BLOCK = 256
TILES_DEV = 2
SEQ_ROWS = 512
GROUPS = 8
P_DEV = 512
M_DEV = 128
CAP = 16
PATCHES = 4096
TILES = 16
MERGE_IN = 5120
RECV_ROWS = 4096
N_SECTION = 2
N_DP = 4


def draw_patch_counts(key, part):
    return (4 * jax.random.randint(key, (TILES,), CAP, BLOCK // 4 + 1)).astype(jnp.int32)


def draw_dest_rows(key, part):
    group_total = GROUPS
    run_total = M_DEV // CAP
    heavy = jax.random.randint(jax.random.fold_in(key, 1), (), 0, group_total).astype(jnp.int32)

    def run_order(order_key):
        others = (heavy + 1 + jax.random.permutation(order_key, group_total - 1).astype(jnp.int32)) % group_total
        return jnp.concatenate([heavy[None], others])[:run_total]
    targets = jax.vmap(run_order)(jax.random.split(jax.random.fold_in(key, 2), group_total))
    places = jax.vmap(lambda place_key: jax.random.permutation(place_key, SEQ_ROWS).astype(jnp.int32))(jax.random.split(jax.random.fold_in(key, 3), group_total))
    source = jnp.arange(group_total, dtype=jnp.int32)[:, None, None]
    lane = jnp.arange(CAP, dtype=jnp.int32)[None, None, :]
    receiver = jnp.broadcast_to(targets[:, :, None], (group_total, run_total, CAP))
    position = places[receiver, source * CAP + lane]
    return (receiver * SEQ_ROWS + position).reshape(-1).astype(jnp.int32)


def draw_qkv_weight(key, part):
    base = jax.random.normal(key, (D_VIT, 3, D_VIT), jnp.float32) * D_VIT ** (-0.5)
    base = jnp.clip(base, -0.15, 0.15)
    return base.astype(jnp.bfloat16)


def draw_section_hidden(key, part):
    noise = jax.random.normal(jax.random.fold_in(key, 1), (RECV_ROWS, HID), jnp.float32)
    column_scale = jnp.exp(jnp.linspace(0.0, math.log(10.0), HID))[None, :]
    row_scale = jnp.exp(jax.random.uniform(jax.random.fold_in(key, 2), (RECV_ROWS, 1), jnp.float32, 0.0, math.log(10.0)))
    return jnp.clip(0.1 * noise * column_scale * row_scale, -80.0, 80.0).astype(jnp.bfloat16)


def shard_levels(key, shape, pieces, low, high):
    loudness = 1.0
    for axis_at, blocks in pieces:
        draws = jax.random.uniform(jax.random.fold_in(jax.random.fold_in(key, 6), axis_at), (blocks,), jnp.float32, low / len(pieces), high / len(pieces))
        loudness = loudness * jnp.repeat(jnp.exp(draws), shape[axis_at] // blocks).reshape((-1,) + (1,) * (len(shape) - 1 - axis_at))
    return loudness


def gaussian(own_key, dims, scale, bound, shards=(), kind=jnp.bfloat16):
    array = scale * jax.random.normal(own_key, dims, jnp.float32)
    if shards:
        array = array * shard_levels(own_key, dims, shards, -0.22, 0.18)
    return jnp.clip(array, -bound, bound).astype(kind)


def setup_inputs(seed: int = 0) -> dict:
    streams_of = jax.random.split(jax.random.key(seed), 15)
    return {
        "patches": gaussian(streams_of[0], (PATCHES, D_VIT), 1.0, 6.0, ((0, 8),)),
        "patch_counts": draw_patch_counts(jax.random.fold_in(streams_of[14], 71), 0),
        "dest_rows": draw_dest_rows(jax.random.fold_in(streams_of[14], 71), 0),
        "qkv_weight": draw_qkv_weight(jax.random.fold_in(streams_of[14], 71), 0),
        "out_weight": gaussian(streams_of[4], (D_VIT, D_VIT), D_VIT ** -0.5, 0.15625, ((0, 4),)),
        "attn_gain": jnp.clip(1.0 + 0.15 * jax.random.normal(streams_of[5], (D_VIT,), jnp.float32), 0.25, 1.75).astype(jnp.bfloat16),
        "merge_gain": jnp.clip(1.0 + 0.15 * jax.random.normal(streams_of[6], (D_VIT,), jnp.float32), 0.25, 1.75).astype(jnp.bfloat16),
        "fc1_weight": gaussian(streams_of[7], (MERGE_IN, MERGE_HID), MERGE_IN ** -0.5, 0.078125, ((0, 4), (1, 8))),
        "fc1_bias": gaussian(streams_of[8], (MERGE_HID,), 0.5, 3.0, ((0, 8),)),
        "fc2_weight": gaussian(streams_of[9], (MERGE_HID, HID), MERGE_HID ** -0.5, 0.078125, ((0, 8), (1, 4))),
        "fc2_bias": gaussian(streams_of[10], (HID,), 0.5, 3.0, ((0, 4),)),
        "text_embeds": gaussian(streams_of[11], (RECV_ROWS, HID), 1.0, 6.0, ((0, 8), (1, 4))),
        "section_hidden": draw_section_hidden(jax.random.fold_in(streams_of[14], 71), 0),
        "llm_gain": jnp.clip(1.0 + 0.15 * jax.random.normal(streams_of[13], (HID,), jnp.float32), 0.25, 1.75).astype(jnp.bfloat16),
    }


vit_eps = 1e-06
llm_eps = 1e-06

def layer_norm(values, gain):
    centred = values.astype(jnp.float32)
    centred = centred - lax.optimization_barrier(jnp.mean(centred, axis=-1, keepdims=True))
    variance = lax.optimization_barrier(jnp.mean(centred * centred, axis=-1, keepdims=True))
    return centred * lax.rsqrt(variance + vit_eps) * gain.astype(jnp.float32)

def group_embed(group_rows, group_counts, qkv_weight, out_weight, attn_gain, merge_gain, fc1_weight, fc1_bias, fc2_weight, fc2_bias):
    normed_in = layer_norm(group_rows, attn_gain).astype(jnp.bfloat16)
    projections = jnp.dot(normed_in, qkv_weight.reshape(D_VIT, 3 * D_VIT), preferred_element_type=jnp.float32).astype(jnp.bfloat16)
    projections = projections.reshape(TILES_DEV, BLOCK, 3, HEADS, HEAD_DIM).astype(jnp.float32)
    query_part = projections[:, :, 0]
    key_part = projections[:, :, 1]
    value_part = projections[:, :, 2]
    scores = jnp.einsum('tqhd,tkhd->thqk', query_part, key_part) * HEAD_DIM ** (-0.5)
    key_live = jnp.arange(BLOCK, dtype=jnp.int32)[None, None, None, :] < group_counts[:, None, None, None]
    scores = jnp.where(key_live, scores, -1e+30)
    weights = jax.nn.softmax(scores, axis=-1).astype(jnp.bfloat16)
    attended = jnp.einsum('thqk,tkhd->tqhd', weights.astype(jnp.float32), value_part).astype(jnp.bfloat16)
    attended = attended.reshape(P_DEV, D_VIT)
    block_out = (group_rows.astype(jnp.float32) + jnp.dot(attended, out_weight, preferred_element_type=jnp.float32)).astype(jnp.bfloat16)
    merge_in = layer_norm(block_out, merge_gain).astype(jnp.bfloat16).reshape(M_DEV, MERGE_IN)
    hidden = jax.nn.gelu(jnp.dot(merge_in, fc1_weight, preferred_element_type=jnp.float32) + fc1_bias.astype(jnp.float32), approximate=False).astype(jnp.bfloat16)
    return (jnp.dot(hidden, fc2_weight, preferred_element_type=jnp.float32) + fc2_bias.astype(jnp.float32)).astype(jnp.bfloat16)

def reference(patches, patch_counts, dest_rows, qkv_weight, out_weight, attn_gain, merge_gain, fc1_weight, fc1_bias, fc2_weight, fc2_bias, text_embeds, section_hidden, llm_gain):
    group_total = N_SECTION * N_DP
    grouped = patches.reshape(group_total, P_DEV, D_VIT)
    grouped_counts = patch_counts.reshape(group_total, TILES_DEV)

    def one_group(pair):
        return group_embed(pair[0], pair[1], qkv_weight, out_weight, attn_gain, merge_gain, fc1_weight, fc1_bias, fc2_weight, fc2_bias)
    image_embeds = lax.map(one_group, (grouped, grouped_counts)).reshape(group_total * M_DEV, HID)
    slot_in_tile = jnp.arange(group_total * M_DEV, dtype=jnp.int32) % (BLOCK // 4)
    tile_counts = jnp.repeat(patch_counts, BLOCK // 4, total_repeat_length=group_total * M_DEV)
    live = slot_in_tile * 4 < tile_counts
    target_rows = jnp.where(live, dest_rows, group_total * SEQ_ROWS).astype(jnp.int32)
    sequence_embeds = text_embeds.at[target_rows].set(image_embeds, mode='drop')
    sectioned_seq = sequence_embeds.reshape(N_SECTION, N_DP * SEQ_ROWS, HID)
    sectioned_hidden = section_hidden.reshape(N_SECTION, N_DP * SEQ_ROWS, HID)
    entering = jnp.concatenate([sectioned_seq[:1], sectioned_hidden[:-1]], axis=0).reshape(group_total * SEQ_ROWS, HID)
    entering = entering.astype(jnp.float32)
    mean_square = lax.optimization_barrier(jnp.mean(entering * entering, axis=1, keepdims=True))
    layer_inputs = (entering * lax.rsqrt(mean_square + llm_eps) * llm_gain.astype(jnp.float32)).astype(jnp.bfloat16)
    return (sequence_embeds, layer_inputs)
```

```python
import jax
import jax.numpy as jnp
from jax import lax
from jax.sharding import PartitionSpec as P

HEAD_DIM = 80
HID = 8192


vit_eps = 1e-06
llm_eps = 1e-06


def from_behind(value, axis, steps):
    count = lax.axis_size(axis)
    first, last = (max(0, -steps), min(count, count - steps))
    return lax.ppermute(value, axis, [(source, source + steps) for source in range(first, last)])


def layer_norm(values, gain):
    centred = values.astype(jnp.float32)
    centred = centred - jnp.mean(centred, axis=-1, keepdims=True)
    variance = jnp.mean(centred * centred, axis=-1, keepdims=True)
    return centred * lax.rsqrt(variance + vit_eps) * gain.astype(jnp.float32)


def sum_scatter_mp(blocks):
    return lax.psum_scatter(blocks, "mp", scatter_dimension=0, tiled=False).astype(jnp.float32)


def gather_mp(value):
    return lax.all_gather(value, "mp", axis=0, tiled=True)


def total_mp(value):
    return lax.psum(value, "mp")


def gather_groups(value):
    return lax.all_gather(value, ("section", "dp"), axis=0, tiled=True)


def sum_scatter_groups(value):
    return lax.psum_scatter(value, ("section", "dp"), scatter_dimension=0, tiled=True)


def per_device(
    patches,
    patch_counts,
    dest_rows,
    qkv_weight,
    out_weight,
    attn_gain,
    merge_gain,
    fc1_weight,
    fc1_bias,
    fc2_weight,
    fc2_bias,
    text_embeds,
    section_hidden,
    llm_gain,
):
    width = patches.shape[1]
    tile_total = patch_counts.shape[0]
    block_rows = patches.shape[0] // tile_total
    merged_rows = patches.shape[0] // 4
    local_cols = qkv_weight.shape[2]
    local_heads = local_cols // HEAD_DIM
    feature_cols = text_embeds.shape[1]
    seq_rows = text_embeds.shape[0]
    section_count = lax.axis_size("section")
    group_count = section_count * lax.axis_size("dp")
    run_cap = max(2, merged_rows // group_count)
    run_total = merged_rows // run_cap
    run_target = dest_rows.reshape(run_total, run_cap)[:, 0] // seq_rows
    takes = jnp.arange(group_count, dtype=jnp.int32)[:, None] == run_target[None, :]
    slot_in_tile = jnp.arange(merged_rows, dtype=jnp.int32) % (block_rows // 4)
    tile_counts = jnp.repeat(patch_counts, block_rows // 4, total_repeat_length=merged_rows)
    live = slot_in_tile * 4 < tile_counts
    place = jnp.where(live, dest_rows % seq_rows - seq_rows, 0).reshape(run_total, run_cap)
    send_place = jnp.sum(jnp.where(takes[:, :, None], place[None], 0), axis=1) + seq_rows
    got_place = lax.all_to_all(send_place, ("section", "dp"), split_axis=0, concat_axis=0, tiled=True)
    incoming = from_behind(section_hidden, "section", 1)
    normed_in = layer_norm(patches, attn_gain).astype(jnp.bfloat16)
    projections = jnp.dot(
        normed_in, qkv_weight.reshape(width, 3 * local_cols), preferred_element_type=jnp.float32
    ).astype(jnp.bfloat16)
    projections = projections.reshape(tile_total, block_rows, 3, local_heads, HEAD_DIM)
    query_part = projections[:, :, 0]
    key_part = projections[:, :, 1]
    value_part = projections[:, :, 2]
    scores = jnp.einsum(
        "tqhd,tkhd->thqk", query_part, key_part, preferred_element_type=jnp.float32
    ) * HEAD_DIM ** (-0.5)
    key_live = (
        jnp.arange(block_rows, dtype=jnp.int32)[None, None, None, :]
        < patch_counts[:, None, None, None]
    )
    scores = jnp.where(key_live, scores, -1e30)
    weights = jax.nn.softmax(scores, axis=-1).astype(jnp.bfloat16)
    attended = jnp.einsum(
        "thqk,tkhd->tqhd", weights, value_part, preferred_element_type=jnp.float32
    ).astype(jnp.bfloat16)
    attended = attended.reshape(patches.shape[0], local_cols)
    partial_proj = jnp.dot(attended, out_weight, preferred_element_type=jnp.float32)
    position = lax.axis_index("mp")
    own_patch = lax.dynamic_slice_in_dim(
        patches.reshape(merged_rows, 4, width), position, 1, 1
    ).reshape(merged_rows, width)
    own_proj = sum_scatter_mp(
        partial_proj.astype(jnp.bfloat16).reshape(merged_rows, 4, width).transpose(1, 0, 2)
    )
    block_out = (own_patch.astype(jnp.float32) + own_proj).astype(jnp.bfloat16)
    merge_part = layer_norm(block_out, merge_gain).astype(jnp.bfloat16)
    lane_same = jnp.arange(run_cap)[:, None] == jnp.arange(run_cap)[None, :]
    order = (takes[:, None, :, None] & lane_same[None, :, None, :]).reshape(
        group_count * run_cap, merged_rows
    )
    merge_part = jnp.dot(
        order.astype(jnp.bfloat16), merge_part, preferred_element_type=jnp.float32
    ).astype(jnp.bfloat16)
    slot_rows = group_count * run_cap
    gathered = gather_groups(merge_part)
    gathered = (
        gathered.reshape(group_count, group_count, run_cap, width)
        .transpose(1, 0, 2, 3)
        .reshape(group_count * slot_rows, width)
    )
    first_partial = jnp.dot(gathered, fc1_weight, preferred_element_type=jnp.float32)
    mp_count = lax.axis_size("mp")
    first_total = sum_scatter_mp(
        first_partial.astype(jnp.bfloat16).reshape(mp_count, -1, fc1_weight.shape[1])
    )
    hidden_part = jax.nn.gelu(
        first_total + fc1_bias.astype(jnp.float32), approximate=False
    ).astype(jnp.bfloat16)
    hidden = gather_mp(hidden_part)
    second_partial = jnp.dot(hidden, fc2_weight, preferred_element_type=jnp.float32)
    embed_total = sum_scatter_groups(second_partial.astype(jnp.bfloat16)).astype(jnp.float32)
    image_embeds = (embed_total + fc2_bias.astype(jnp.float32)).astype(jnp.bfloat16)
    hits = got_place.reshape(1, -1) == jnp.arange(seq_rows, dtype=jnp.int32)[:, None]
    placed = jnp.dot(
        hits.astype(jnp.bfloat16), image_embeds, preferred_element_type=jnp.float32
    ).astype(jnp.bfloat16)
    sequence_embeds = jnp.where(jnp.any(hits, axis=1)[:, None], placed, text_embeds)
    entering = jnp.where(lax.axis_index("section") == 0, sequence_embeds, incoming).astype(
        jnp.float32
    )
    row_total = total_mp(jnp.sum(entering * entering, axis=1))
    layer_inputs = (
        entering * lax.rsqrt(row_total / HID + llm_eps)[:, None] * llm_gain.astype(jnp.float32)
    ).astype(jnp.bfloat16)
    return (sequence_embeds, layer_inputs)


def solution(mesh):
    in_specs = (
        P(("section", "dp"), None),
        P(("section", "dp")),
        P(("section", "dp")),
        P(None, None, "mp"),
        P("mp", None),
        P(),
        P(),
        P("mp", ("section", "dp")),
        P(("section", "dp")),
        P(("section", "dp"), "mp"),
        P("mp"),
        P(("section", "dp"), "mp"),
        P(("section", "dp"), "mp"),
        P("mp"),
    )
    out_specs = (P(("section", "dp"), "mp"), P(("section", "dp"), "mp"))
    return jax.shard_map(
        per_device, mesh=mesh, in_specs=in_specs, out_specs=out_specs, check_vma=False
    )
```

```python
import functools
import math

import jax
import jax.numpy as jnp
from jax import lax
from jax.experimental import pallas as pl
from jax.experimental.pallas import tpu as pltpu
from jax.sharding import PartitionSpec as P

HEAD_DIM = 80
HID = 8192


vit_eps = 1e-06
llm_eps = 1e-06


def from_behind(value, axis, steps):
    count = lax.axis_size(axis)
    first, last = (max(0, -steps), min(count, count - steps))
    return lax.ppermute(value, axis, [(source, source + steps) for source in range(first, last)])


def layer_norm(values, gain):
    centred = values.astype(jnp.float32)
    centred = centred - jnp.mean(centred, axis=-1, keepdims=True)
    variance = jnp.mean(centred * centred, axis=-1, keepdims=True)
    return centred * lax.rsqrt(variance + vit_eps) * gain.astype(jnp.float32)


VMEM_LIMIT = 60 * 1024 * 1024
KERNEL_BYTES = 8 * 1024 * 1024


def vmem_call(kernel, out, scratch, sent_bytes, ident, *operands):
    return pl.pallas_call(
        kernel,
        out_shape=out,
        in_specs=[pl.BlockSpec(memory_space=pltpu.VMEM)] * len(operands),
        out_specs=pl.BlockSpec(memory_space=pltpu.VMEM),
        scratch_shapes=scratch,
        cost_estimate=pl.CostEstimate(
            flops=sent_bytes * 20000, bytes_accessed=sent_bytes * 2, transcendentals=0
        ),
        compiler_params=pltpu.CompilerParams(
            collective_id=ident, has_side_effects=True, vmem_limit_bytes=VMEM_LIMIT
        ),
    )(*operands)


def exchange_kernel(count, spread, x_ref, o_ref, send_sem, recv_sem, own_sem):
    me = lax.axis_index("mp")
    barrier = pltpu.get_barrier_semaphore()
    for step in range(1, count):
        peer = lax.rem(me + step, count)
        pl.semaphore_signal(
            barrier, inc=1, device_id={"mp": peer}, device_id_type=pl.DeviceIdType.MESH
        )
    pl.semaphore_wait(barrier, count - 1)
    copies = []
    for step in sorted(range(1, count), key=lambda s: -min(s, count - s)):
        peer = lax.rem(me + step, count)
        copy = pltpu.make_async_remote_copy(
            src_ref=x_ref.at[peer] if spread else x_ref,
            dst_ref=o_ref.at[me],
            send_sem=send_sem.at[step - 1],
            recv_sem=recv_sem.at[step - 1],
            device_id={"mp": peer},
            device_id_type=pl.DeviceIdType.MESH,
        )
        copy.start()
        copies.append(copy)
    own = pltpu.make_async_copy(x_ref.at[me] if spread else x_ref, o_ref.at[me], own_sem)
    own.start()
    own.wait()
    for copy in copies:
        copy.wait()


def exchange_mp(value, spread, ident):
    count = lax.axis_size("mp")
    shape = value.shape if spread else (count,) + value.shape
    size = math.prod(shape) * value.dtype.itemsize
    return vmem_call(
        functools.partial(exchange_kernel, count, spread),
        jax.ShapeDtypeStruct(shape, value.dtype),
        [
            pltpu.SemaphoreType.DMA((count - 1,)),
            pltpu.SemaphoreType.DMA((count - 1,)),
            pltpu.SemaphoreType.DMA,
        ],
        size,
        ident,
        value,
    )


def sum_scatter_mp(blocks, ident):
    return jnp.sum(exchange_mp(blocks, True, ident).astype(jnp.float32), axis=0)


def gather_mp(value):
    got = exchange_mp(value, False, 2)
    return got.reshape((-1,) + value.shape[1:])


def total_mp(value):
    return jnp.sum(exchange_mp(value.reshape(-1, 128), False, 3), axis=0).reshape(-1)


def flip(index, bit):
    return index + bit * (1 - 2 * (index // bit % 2))


def group_bits():
    outer = [("dp", 1 << k) for k in range(1, lax.axis_size("dp").bit_length() - 1)]
    outer += [("section", 1 << k) for k in range(lax.axis_size("section").bit_length() - 1)]
    return outer, ("dp", 1)


def meets(axis, bit):
    return {axis: flip(lax.axis_index(axis), bit)}


def group_at(mask):
    spots = {axis: lax.axis_index(axis) for axis in ("section", "dp")}
    for axis, bit in mask:
        spots[axis] = flip(spots[axis], bit)
    return spots["section"] * lax.axis_size("dp") + spots["dp"]


def greet(bits):
    barrier = pltpu.get_barrier_semaphore()
    for axis, bit in bits:
        pl.semaphore_signal(
            barrier, inc=1, device_id=meets(axis, bit), device_id_type=pl.DeviceIdType.MESH
        )
    pl.semaphore_wait(barrier, len(bits))


def gather_kernel(x_ref, o_ref, send_sem, recv_sem, own_sem):
    outer, last = group_bits()
    greet(outer + [last])
    half = x_ref.shape[1] // 2
    sent, waiting = [], []
    slots = iter(range(send_sem.shape[0]))

    def pass_on(mask, stage, part, order):
        cols = pl.ds(part * half, half)
        spot = group_at(mask)
        source = o_ref.at[spot, :, cols] if mask else x_ref.at[:, cols]
        for later in range(stage, len(order)):
            slot = next(slots)
            copy = pltpu.make_async_remote_copy(
                src_ref=source,
                dst_ref=o_ref.at[spot, :, cols],
                send_sem=send_sem.at[slot],
                recv_sem=recv_sem.at[slot],
                device_id=meets(*order[later]),
                device_id_type=pl.DeviceIdType.MESH,
            )
            copy.start()
            sent.append(copy)
            waiting.append((later, copy, mask + [order[later]], part, order))

    pass_on([], 0, 0, outer + [last])
    pass_on([], 0, 1, outer[::-1] + [last])
    own = pltpu.make_async_copy(x_ref, o_ref.at[group_at([])], own_sem)
    own.start()
    while waiting:
        first = min(range(len(waiting)), key=lambda at: waiting[at][0])
        stage, copy, mask, part, order = waiting.pop(first)
        copy.wait_recv()
        pass_on(mask, stage + 1, part, order)
    for copy in sent:
        copy.wait_send()
    own.wait()


def gather_groups(value):
    count = lax.axis_size("section") * lax.axis_size("dp")
    size = count * value.size * value.dtype.itemsize
    if size > KERNEL_BYTES:
        return lax.all_gather(value, ("section", "dp"), axis=0, tiled=True)
    slots = 2 * (count - 1)
    got = vmem_call(
        gather_kernel,
        jax.ShapeDtypeStruct((count,) + value.shape, value.dtype),
        [
            pltpu.SemaphoreType.DMA((slots,)),
            pltpu.SemaphoreType.DMA((slots,)),
            pltpu.SemaphoreType.DMA,
        ],
        size,
        4,
        value,
    )
    return got.reshape(-1, value.shape[1])


def scatter_kernel(x_ref, o_ref, held, taken, send_sem, recv_sem):
    outer, first = group_bits()
    greet(outer + [first])
    rows = x_ref.shape[1]
    half = x_ref.shape[2] // 2
    chunk = 32
    orders = ([first] + outer, [first] + outer[::-1])
    slots = iter(range(send_sem.shape[0]))
    masks = [[]]
    for bit in outer:
        masks = masks + [mask + [bit] for mask in masks]
    place_of = {frozenset(mask): at for at, mask in enumerate(masks)}
    base = len(masks)
    live = {}

    def send(part, stage):
        cols = pl.ds(part * half, half)
        bit = orders[part][stage]
        kept = orders[part][stage + 1 :]
        copies = []
        for mask in [m for m in masks if set(m) <= set(kept)]:
            if stage == 0:
                source = x_ref.at[group_at(mask + [bit]), :, cols]
            else:
                source = held.at[place_of[frozenset(mask + [bit])], :, cols]
            landing = 2 * base - 2 ** (len(kept) + 1) + [
                m for m in masks if set(m) <= set(kept)
            ].index(mask)
            slot = next(slots)
            copy = pltpu.make_async_remote_copy(
                src_ref=source,
                dst_ref=taken.at[landing, :, cols],
                send_sem=send_sem.at[slot],
                recv_sem=recv_sem.at[slot],
                device_id=meets(*bit),
                device_id_type=pl.DeviceIdType.MESH,
            )
            copy.start()
            copies.append((copy, mask, landing))
        live[part, stage] = copies

    def add(part, stage):
        cols = pl.ds(part * half, half)
        final = stage + 1 == len(orders[part])
        following = None if final else orders[part][stage + 1]
        copies = live[part, stage]
        for copy, mask, landing in sorted(copies, key=lambda c: following not in c[1]):
            copy.wait_recv()
            at = place_of[frozenset(mask)]
            spot = group_at(mask)

            @pl.loop(0, rows // chunk)
            def _(step):
                span = pl.ds(step * chunk, chunk)
                mine = x_ref[spot, span, cols] if stage == 0 else held[at, span, cols]
                total = mine.astype(jnp.float32) + taken[landing, span, cols].astype(jnp.float32)
                if final:
                    o_ref[span, cols] = total
                else:
                    held[at, span, cols] = total.astype(held.dtype)

    send(0, 0)
    send(1, 0)
    for stage in range(len(orders[0])):
        for part in (0, 1):
            add(part, stage)
            if stage + 1 < len(orders[0]):
                send(part, stage + 1)
    for copies in live.values():
        for copy, _, _ in copies:
            copy.wait_send()


def sum_scatter_groups(value):
    count = lax.axis_size("section") * lax.axis_size("dp")
    size = value.size * value.dtype.itemsize
    if size > KERNEL_BYTES:
        return lax.psum_scatter(value, ("section", "dp"), scatter_dimension=0, tiled=True)
    rows, cols = value.shape[0] // count, value.shape[1]
    slots = 2 * (count - 1)
    return vmem_call(
        scatter_kernel,
        jax.ShapeDtypeStruct((rows, cols), jnp.float32),
        [
            pltpu.VMEM((count // 2, rows, cols), value.dtype),
            pltpu.VMEM((count - 1, rows, cols), value.dtype),
            pltpu.SemaphoreType.DMA((slots,)),
            pltpu.SemaphoreType.DMA((slots,)),
        ],
        size,
        5,
        value.reshape(count, rows, cols),
    )


def per_device(
    patches,
    patch_counts,
    dest_rows,
    qkv_weight,
    out_weight,
    attn_gain,
    merge_gain,
    fc1_weight,
    fc1_bias,
    fc2_weight,
    fc2_bias,
    text_embeds,
    section_hidden,
    llm_gain,
):
    width = patches.shape[1]
    tile_total = patch_counts.shape[0]
    block_rows = patches.shape[0] // tile_total
    merged_rows = patches.shape[0] // 4
    local_cols = qkv_weight.shape[2]
    local_heads = local_cols // HEAD_DIM
    feature_cols = text_embeds.shape[1]
    seq_rows = text_embeds.shape[0]
    section_count = lax.axis_size("section")
    group_count = section_count * lax.axis_size("dp")
    run_cap = max(2, merged_rows // group_count)
    run_total = merged_rows // run_cap
    run_target = dest_rows.reshape(run_total, run_cap)[:, 0] // seq_rows
    takes = jnp.arange(group_count, dtype=jnp.int32)[:, None] == run_target[None, :]
    slot_in_tile = jnp.arange(merged_rows, dtype=jnp.int32) % (block_rows // 4)
    tile_counts = jnp.repeat(patch_counts, block_rows // 4, total_repeat_length=merged_rows)
    live = slot_in_tile * 4 < tile_counts
    place = jnp.where(live, dest_rows % seq_rows - seq_rows, 0).reshape(run_total, run_cap)
    send_place = jnp.sum(jnp.where(takes[:, :, None], place[None], 0), axis=1) + seq_rows
    got_place = lax.all_to_all(send_place, ("section", "dp"), split_axis=0, concat_axis=0, tiled=True)
    incoming = from_behind(section_hidden, "section", 1)
    normed_in = layer_norm(patches, attn_gain).astype(jnp.bfloat16)
    projections = jnp.dot(
        normed_in, qkv_weight.reshape(width, 3 * local_cols), preferred_element_type=jnp.float32
    ).astype(jnp.bfloat16)
    projections = projections.reshape(tile_total, block_rows, 3, local_heads, HEAD_DIM)
    query_part = projections[:, :, 0]
    key_part = projections[:, :, 1]
    value_part = projections[:, :, 2]
    scores = jnp.einsum(
        "tqhd,tkhd->thqk", query_part, key_part, preferred_element_type=jnp.float32
    ) * HEAD_DIM ** (-0.5)
    key_live = (
        jnp.arange(block_rows, dtype=jnp.int32)[None, None, None, :]
        < patch_counts[:, None, None, None]
    )
    scores = jnp.where(key_live, scores, -1e30)
    weights = jax.nn.softmax(scores, axis=-1).astype(jnp.bfloat16)
    attended = jnp.einsum(
        "thqk,tkhd->tqhd", weights, value_part, preferred_element_type=jnp.float32
    ).astype(jnp.bfloat16)
    attended = attended.reshape(patches.shape[0], local_cols)
    partial_proj = jnp.dot(attended, out_weight, preferred_element_type=jnp.float32)
    position = lax.axis_index("mp")
    own_patch = lax.dynamic_slice_in_dim(
        patches.reshape(merged_rows, 4, width), position, 1, 1
    ).reshape(merged_rows, width)
    own_proj = sum_scatter_mp(
        partial_proj.astype(jnp.bfloat16).reshape(merged_rows, 4, width).transpose(1, 0, 2),
        0,
    )
    block_out = (own_patch.astype(jnp.float32) + own_proj).astype(jnp.bfloat16)
    merge_part = layer_norm(block_out, merge_gain).astype(jnp.bfloat16)
    lane_same = jnp.arange(run_cap)[:, None] == jnp.arange(run_cap)[None, :]
    order = (takes[:, None, :, None] & lane_same[None, :, None, :]).reshape(
        group_count * run_cap, merged_rows
    )
    merge_part = jnp.dot(
        order.astype(jnp.bfloat16), merge_part, preferred_element_type=jnp.float32
    ).astype(jnp.bfloat16)
    slot_rows = group_count * run_cap
    gathered = gather_groups(merge_part)
    gathered = (
        gathered.reshape(group_count, group_count, run_cap, width)
        .transpose(1, 0, 2, 3)
        .reshape(group_count * slot_rows, width)
    )
    first_partial = jnp.dot(gathered, fc1_weight, preferred_element_type=jnp.float32)
    mp_count = lax.axis_size("mp")
    first_total = sum_scatter_mp(
        first_partial.astype(jnp.bfloat16).reshape(mp_count, -1, fc1_weight.shape[1]),
        1,
    )
    hidden_part = jax.nn.gelu(
        first_total + fc1_bias.astype(jnp.float32), approximate=False
    ).astype(jnp.bfloat16)
    hidden = gather_mp(hidden_part)
    second_partial = jnp.dot(hidden, fc2_weight, preferred_element_type=jnp.float32)
    embed_total = sum_scatter_groups(second_partial.astype(jnp.bfloat16)).astype(jnp.float32)
    image_embeds = (embed_total + fc2_bias.astype(jnp.float32)).astype(jnp.bfloat16)
    hits = got_place.reshape(1, -1) == jnp.arange(seq_rows, dtype=jnp.int32)[:, None]
    placed = jnp.dot(
        hits.astype(jnp.bfloat16), image_embeds, preferred_element_type=jnp.float32
    ).astype(jnp.bfloat16)
    sequence_embeds = jnp.where(jnp.any(hits, axis=1)[:, None], placed, text_embeds)
    entering = jnp.where(lax.axis_index("section") == 0, sequence_embeds, incoming).astype(
        jnp.float32
    )
    row_total = total_mp(jnp.sum(entering * entering, axis=1))
    layer_inputs = (
        entering * lax.rsqrt(row_total / HID + llm_eps)[:, None] * llm_gain.astype(jnp.float32)
    ).astype(jnp.bfloat16)
    return (sequence_embeds, layer_inputs)


def solution(mesh):
    in_specs = (
        P(("section", "dp"), None),
        P(("section", "dp")),
        P(("section", "dp")),
        P(None, None, "mp"),
        P("mp", None),
        P(),
        P(),
        P("mp", ("section", "dp")),
        P(("section", "dp")),
        P(("section", "dp"), "mp"),
        P("mp"),
        P(("section", "dp"), "mp"),
        P(("section", "dp"), "mp"),
        P("mp"),
    )
    out_specs = (P(("section", "dp"), "mp"), P(("section", "dp"), "mp"))
    return jax.shard_map(
        per_device, mesh=mesh, in_specs=in_specs, out_specs=out_specs, check_vma=False
    )
```

```python
import functools
import math

import jax
import jax.numpy as jnp
from jax import lax
from jax.experimental import pallas as pl
from jax.experimental.pallas import tpu as pltpu
from jax.sharding import PartitionSpec as P

HEAD_DIM = 80
HID = 8192


vit_eps = 1e-06
llm_eps = 1e-06


def from_behind(value, axis, steps):
    count = lax.axis_size(axis)
    first, last = (max(0, -steps), min(count, count - steps))
    return lax.ppermute(value, axis, [(source, source + steps) for source in range(first, last)])


def layer_norm(values, gain):
    centred = values.astype(jnp.float32)
    centred = centred - jnp.mean(centred, axis=-1, keepdims=True)
    variance = jnp.mean(centred * centred, axis=-1, keepdims=True)
    return centred * lax.rsqrt(variance + vit_eps) * gain.astype(jnp.float32)


VMEM_LIMIT = 60 * 1024 * 1024
KERNEL_BYTES = 8 * 1024 * 1024


def vmem_call(kernel, out, scratch, sent_bytes, ident, *operands):
    return pl.pallas_call(
        kernel,
        out_shape=out,
        in_specs=[pl.BlockSpec(memory_space=pltpu.VMEM)] * len(operands),
        out_specs=pl.BlockSpec(memory_space=pltpu.VMEM),
        scratch_shapes=scratch,
        cost_estimate=pl.CostEstimate(
            flops=sent_bytes * 20000, bytes_accessed=sent_bytes * 2, transcendentals=0
        ),
        compiler_params=pltpu.CompilerParams(
            collective_id=ident, has_side_effects=True, vmem_limit_bytes=VMEM_LIMIT
        ),
    )(*operands)


def exchange_kernel(count, spread, x_ref, o_ref, send_sem, recv_sem, own_sem):
    me = lax.axis_index("mp")
    barrier = pltpu.get_barrier_semaphore()
    for step in range(1, count):
        peer = lax.rem(me + step, count)
        pl.semaphore_signal(
            barrier, inc=1, device_id={"mp": peer}, device_id_type=pl.DeviceIdType.MESH
        )
    pl.semaphore_wait(barrier, count - 1)
    copies = []
    for step in sorted(range(1, count), key=lambda s: -min(s, count - s)):
        peer = lax.rem(me + step, count)
        copy = pltpu.make_async_remote_copy(
            src_ref=x_ref.at[peer] if spread else x_ref,
            dst_ref=o_ref.at[me],
            send_sem=send_sem.at[step - 1],
            recv_sem=recv_sem.at[step - 1],
            device_id={"mp": peer},
            device_id_type=pl.DeviceIdType.MESH,
        )
        copy.start()
        copies.append(copy)
    own = pltpu.make_async_copy(x_ref.at[me] if spread else x_ref, o_ref.at[me], own_sem)
    own.start()
    own.wait()
    for copy in copies:
        copy.wait()


def relay_kernel(count, x_ref, o_ref, send_sem, recv_sem, own_sem):
    me = lax.axis_index("mp")
    barrier = pltpu.get_barrier_semaphore()
    for step in range(1, count):
        peer = lax.rem(me + step, count)
        pl.semaphore_signal(
            barrier, inc=1, device_id={"mp": peer}, device_id_type=pl.DeviceIdType.MESH
        )
    pl.semaphore_wait(barrier, count - 1)
    own = pltpu.make_async_copy(x_ref, o_ref.at[me], own_sem)
    own.start()

    def hop(way, step):
        owner = lax.rem(me - way * step + count, count)
        return pltpu.make_async_remote_copy(
            src_ref=o_ref.at[owner] if step else x_ref,
            dst_ref=o_ref.at[owner],
            send_sem=send_sem.at[(way + 1) // 2, step],
            recv_sem=recv_sem.at[(way + 1) // 2, step],
            device_id={"mp": lax.rem(me + way + count, count)},
            device_id_type=pl.DeviceIdType.MESH,
        )

    def holds(way, step):
        return me >= step if way > 0 else me + step < count

    def sends(way):
        return me < count - 1 if way > 0 else me > 0

    for step in range(count):
        for way in (1, -1):
            if step:

                @pl.when(holds(way, step))
                def _():
                    owner = lax.rem(me - way * step + count, count)
                    pltpu.make_async_remote_copy(
                        src_ref=x_ref,
                        dst_ref=o_ref.at[owner],
                        send_sem=send_sem.at[(way + 1) // 2, step - 1],
                        recv_sem=recv_sem.at[(way + 1) // 2, step - 1],
                        device_id={"mp": lax.rem(me - way + count, count)},
                        device_id_type=pl.DeviceIdType.MESH,
                    ).wait_recv()

            if step < count - 1:

                @pl.when(jnp.logical_and(holds(way, step), sends(way)))
                def _():
                    hop(way, step).start()

    own.wait()
    for step in range(count - 1):
        for way in (1, -1):

            @pl.when(jnp.logical_and(holds(way, step), sends(way)))
            def _():
                hop(way, step).wait_send()


def relay_mp(value, ident):
    count = lax.axis_size("mp")
    return vmem_call(
        functools.partial(relay_kernel, count),
        jax.ShapeDtypeStruct((count,) + value.shape, value.dtype),
        [
            pltpu.SemaphoreType.DMA((2, count - 1)),
            pltpu.SemaphoreType.DMA((2, count - 1)),
            pltpu.SemaphoreType.DMA,
        ],
        count * value.size * value.dtype.itemsize,
        ident,
        value,
    )


def exchange_mp(value, spread, ident):
    count = lax.axis_size("mp")
    shape = value.shape if spread else (count,) + value.shape
    size = math.prod(shape) * value.dtype.itemsize
    return vmem_call(
        functools.partial(exchange_kernel, count, spread),
        jax.ShapeDtypeStruct(shape, value.dtype),
        [
            pltpu.SemaphoreType.DMA((count - 1,)),
            pltpu.SemaphoreType.DMA((count - 1,)),
            pltpu.SemaphoreType.DMA,
        ],
        size,
        ident,
        value,
    )


def sum_scatter_mp(blocks, ident):
    return jnp.sum(exchange_mp(blocks, True, ident).astype(jnp.float32), axis=0)


def gather_mp(value):
    got = relay_mp(value, 2)
    return got.reshape((-1,) + value.shape[1:])


def total_mp(value):
    return jnp.sum(exchange_mp(value.reshape(-1, 128), False, 3), axis=0).reshape(-1)


def flip(index, bit):
    return index + bit * (1 - 2 * (index // bit % 2))


def group_bits():
    outer = [("dp", 1 << k) for k in range(1, lax.axis_size("dp").bit_length() - 1)]
    outer += [("section", 1 << k) for k in range(lax.axis_size("section").bit_length() - 1)]
    return outer, ("dp", 1)


def meets(axis, bit):
    return {axis: flip(lax.axis_index(axis), bit)}


def group_at(mask):
    spots = {axis: lax.axis_index(axis) for axis in ("section", "dp")}
    for axis, bit in mask:
        spots[axis] = flip(spots[axis], bit)
    return spots["section"] * lax.axis_size("dp") + spots["dp"]


def greet(bits):
    barrier = pltpu.get_barrier_semaphore()
    for axis, bit in bits:
        pl.semaphore_signal(
            barrier, inc=1, device_id=meets(axis, bit), device_id_type=pl.DeviceIdType.MESH
        )
    pl.semaphore_wait(barrier, len(bits))


def gather_kernel(x_ref, o_ref, send_sem, recv_sem, own_sem):
    outer, last = group_bits()
    greet(outer + [last])
    half = x_ref.shape[1] // 2
    sent, waiting = [], []
    slots = iter(range(send_sem.shape[0]))

    def pass_on(mask, stage, part, order):
        cols = pl.ds(part * half, half)
        spot = group_at(mask)
        source = o_ref.at[spot, :, cols] if mask else x_ref.at[:, cols]
        for later in range(stage, len(order)):
            slot = next(slots)
            copy = pltpu.make_async_remote_copy(
                src_ref=source,
                dst_ref=o_ref.at[spot, :, cols],
                send_sem=send_sem.at[slot],
                recv_sem=recv_sem.at[slot],
                device_id=meets(*order[later]),
                device_id_type=pl.DeviceIdType.MESH,
            )
            copy.start()
            sent.append(copy)
            waiting.append((later, copy, mask + [order[later]], part, order))

    pass_on([], 0, 0, outer + [last])
    pass_on([], 0, 1, outer[::-1] + [last])
    own = pltpu.make_async_copy(x_ref, o_ref.at[group_at([])], own_sem)
    own.start()
    while waiting:
        first = min(range(len(waiting)), key=lambda at: waiting[at][0])
        stage, copy, mask, part, order = waiting.pop(first)
        copy.wait_recv()
        pass_on(mask, stage + 1, part, order)
    for copy in sent:
        copy.wait_send()
    own.wait()


def gather_groups(value):
    count = lax.axis_size("section") * lax.axis_size("dp")
    size = count * value.size * value.dtype.itemsize
    if size > KERNEL_BYTES:
        return lax.all_gather(value, ("section", "dp"), axis=0, tiled=True)
    slots = 2 * (count - 1)
    got = vmem_call(
        gather_kernel,
        jax.ShapeDtypeStruct((count,) + value.shape, value.dtype),
        [
            pltpu.SemaphoreType.DMA((slots,)),
            pltpu.SemaphoreType.DMA((slots,)),
            pltpu.SemaphoreType.DMA,
        ],
        size,
        4,
        value,
    )
    return got.reshape(-1, value.shape[1])


def scatter_kernel(x_ref, o_ref, held, taken, send_sem, recv_sem):
    outer, first = group_bits()
    greet(outer + [first])
    rows = x_ref.shape[1]
    half = x_ref.shape[2] // 2
    chunk = 32
    orders = ([first] + outer, [first] + outer[::-1])
    slots = iter(range(send_sem.shape[0]))
    masks = [[]]
    for bit in outer:
        masks = masks + [mask + [bit] for mask in masks]
    place_of = {frozenset(mask): at for at, mask in enumerate(masks)}
    base = len(masks)
    live = {}

    def send(part, stage):
        cols = pl.ds(part * half, half)
        bit = orders[part][stage]
        kept = orders[part][stage + 1 :]
        copies = []
        for mask in [m for m in masks if set(m) <= set(kept)]:
            if stage == 0:
                source = x_ref.at[group_at(mask + [bit]), :, cols]
            else:
                source = held.at[place_of[frozenset(mask + [bit])], :, cols]
            landing = 2 * base - 2 ** (len(kept) + 1) + [
                m for m in masks if set(m) <= set(kept)
            ].index(mask)
            slot = next(slots)
            copy = pltpu.make_async_remote_copy(
                src_ref=source,
                dst_ref=taken.at[landing, :, cols],
                send_sem=send_sem.at[slot],
                recv_sem=recv_sem.at[slot],
                device_id=meets(*bit),
                device_id_type=pl.DeviceIdType.MESH,
            )
            copy.start()
            copies.append((copy, mask, landing))
        live[part, stage] = copies

    def add(part, stage):
        cols = pl.ds(part * half, half)
        final = stage + 1 == len(orders[part])
        following = None if final else orders[part][stage + 1]
        copies = live[part, stage]
        for copy, mask, landing in sorted(copies, key=lambda c: following not in c[1]):
            copy.wait_recv()
            at = place_of[frozenset(mask)]
            spot = group_at(mask)

            @pl.loop(0, rows // chunk)
            def _(step):
                span = pl.ds(step * chunk, chunk)
                mine = x_ref[spot, span, cols] if stage == 0 else held[at, span, cols]
                total = mine.astype(jnp.float32) + taken[landing, span, cols].astype(jnp.float32)
                if final:
                    o_ref[span, cols] = total
                else:
                    held[at, span, cols] = total.astype(held.dtype)

    send(0, 0)
    send(1, 0)
    for stage in range(len(orders[0])):
        for part in (0, 1):
            add(part, stage)
            if stage + 1 < len(orders[0]):
                send(part, stage + 1)
    for copies in live.values():
        for copy, _, _ in copies:
            copy.wait_send()


def sum_scatter_groups(value):
    count = lax.axis_size("section") * lax.axis_size("dp")
    size = value.size * value.dtype.itemsize
    if size > KERNEL_BYTES:
        return lax.psum_scatter(value, ("section", "dp"), scatter_dimension=0, tiled=True)
    rows, cols = value.shape[0] // count, value.shape[1]
    slots = 2 * (count - 1)
    return vmem_call(
        scatter_kernel,
        jax.ShapeDtypeStruct((rows, cols), jnp.float32),
        [
            pltpu.VMEM((count // 2, rows, cols), value.dtype),
            pltpu.VMEM((count - 1, rows, cols), value.dtype),
            pltpu.SemaphoreType.DMA((slots,)),
            pltpu.SemaphoreType.DMA((slots,)),
        ],
        size,
        5,
        value.reshape(count, rows, cols),
    )


def per_device(
    patches,
    patch_counts,
    dest_rows,
    qkv_weight,
    out_weight,
    attn_gain,
    merge_gain,
    fc1_weight,
    fc1_bias,
    fc2_weight,
    fc2_bias,
    text_embeds,
    section_hidden,
    llm_gain,
):
    width = patches.shape[1]
    tile_total = patch_counts.shape[0]
    block_rows = patches.shape[0] // tile_total
    merged_rows = patches.shape[0] // 4
    local_cols = qkv_weight.shape[2]
    local_heads = local_cols // HEAD_DIM
    feature_cols = text_embeds.shape[1]
    seq_rows = text_embeds.shape[0]
    section_count = lax.axis_size("section")
    group_count = section_count * lax.axis_size("dp")
    run_cap = max(2, merged_rows // group_count)
    run_total = merged_rows // run_cap
    run_target = dest_rows.reshape(run_total, run_cap)[:, 0] // seq_rows
    takes = jnp.arange(group_count, dtype=jnp.int32)[:, None] == run_target[None, :]
    slot_in_tile = jnp.arange(merged_rows, dtype=jnp.int32) % (block_rows // 4)
    tile_counts = jnp.repeat(patch_counts, block_rows // 4, total_repeat_length=merged_rows)
    live = slot_in_tile * 4 < tile_counts
    place = jnp.where(live, dest_rows % seq_rows - seq_rows, 0).reshape(run_total, run_cap)
    send_place = jnp.sum(jnp.where(takes[:, :, None], place[None], 0), axis=1) + seq_rows
    got_place = lax.all_to_all(send_place, ("section", "dp"), split_axis=0, concat_axis=0, tiled=True)
    incoming = from_behind(section_hidden, "section", 1)
    normed_in = layer_norm(patches, attn_gain).astype(jnp.bfloat16)
    projections = jnp.dot(
        normed_in, qkv_weight.reshape(width, 3 * local_cols), preferred_element_type=jnp.float32
    ).astype(jnp.bfloat16)
    projections = projections.reshape(tile_total, block_rows, 3, local_heads, HEAD_DIM)
    query_part = projections[:, :, 0]
    key_part = projections[:, :, 1]
    value_part = projections[:, :, 2]
    scores = jnp.einsum(
        "tqhd,tkhd->thqk", query_part, key_part, preferred_element_type=jnp.float32
    ) * HEAD_DIM ** (-0.5)
    key_live = (
        jnp.arange(block_rows, dtype=jnp.int32)[None, None, None, :]
        < patch_counts[:, None, None, None]
    )
    scores = jnp.where(key_live, scores, -1e30)
    weights = jax.nn.softmax(scores, axis=-1).astype(jnp.bfloat16)
    attended = jnp.einsum(
        "thqk,tkhd->tqhd", weights, value_part, preferred_element_type=jnp.float32
    ).astype(jnp.bfloat16)
    attended = attended.reshape(patches.shape[0], local_cols)
    lane_source = jnp.arange(run_total, dtype=jnp.int32)[None, :] * run_cap
    run_source = jnp.sum(jnp.where(takes, lane_source, 0), axis=1)
    row_source = (
        run_source[:, None] + jnp.arange(run_cap, dtype=jnp.int32)[None, :]
    ).reshape(-1) * 4
    slots_at = jnp.arange(patches.shape[0], dtype=jnp.int32)
    patch_at = jnp.arange(4, dtype=jnp.int32)
    order = (
        (row_source[None, :] + patch_at[:, None]).reshape(-1)[:, None] == slots_at[None, :]
    ).astype(jnp.bfloat16)
    own_order = (
        (row_source + lax.axis_index("mp"))[:, None] == slots_at[None, :]
    ).astype(jnp.bfloat16)
    ordered = jnp.dot(order, attended, preferred_element_type=jnp.float32).astype(jnp.bfloat16)
    own_patch = jnp.dot(own_order, patches, preferred_element_type=jnp.float32)
    partial_proj = jnp.dot(ordered, out_weight, preferred_element_type=jnp.float32)
    own_proj = sum_scatter_mp(
        partial_proj.astype(jnp.bfloat16).reshape(4, group_count * run_cap, width), 0
    )
    block_out = (own_patch + own_proj).astype(jnp.bfloat16)
    merge_part = layer_norm(block_out, merge_gain).astype(jnp.bfloat16)
    slot_rows = group_count * run_cap
    gathered = gather_groups(merge_part)
    gathered = (
        gathered.reshape(group_count, group_count, run_cap, width)
        .transpose(1, 0, 2, 3)
        .reshape(group_count * slot_rows, width)
    )
    first_partial = jnp.dot(gathered, fc1_weight, preferred_element_type=jnp.float32)
    mp_count = lax.axis_size("mp")
    first_total = sum_scatter_mp(
        first_partial.astype(jnp.bfloat16).reshape(mp_count, -1, fc1_weight.shape[1]),
        1,
    )
    hidden_part = jax.nn.gelu(
        first_total + fc1_bias.astype(jnp.float32), approximate=False
    ).astype(jnp.bfloat16)
    hidden = gather_mp(hidden_part)
    second_partial = jnp.dot(hidden, fc2_weight, preferred_element_type=jnp.float32)
    embed_total = sum_scatter_groups(second_partial.astype(jnp.bfloat16)).astype(jnp.float32)
    image_embeds = (embed_total + fc2_bias.astype(jnp.float32)).astype(jnp.bfloat16)
    hits = got_place.reshape(1, -1) == jnp.arange(seq_rows, dtype=jnp.int32)[:, None]
    placed = jnp.dot(
        hits.astype(jnp.bfloat16), image_embeds, preferred_element_type=jnp.float32
    ).astype(jnp.bfloat16)
    sequence_embeds = jnp.where(jnp.any(hits, axis=1)[:, None], placed, text_embeds)
    entering = jnp.where(lax.axis_index("section") == 0, sequence_embeds, incoming).astype(
        jnp.float32
    )
    row_total = total_mp(jnp.sum(entering * entering, axis=1))
    layer_inputs = (
        entering * lax.rsqrt(row_total / HID + llm_eps)[:, None] * llm_gain.astype(jnp.float32)
    ).astype(jnp.bfloat16)
    return (sequence_embeds, layer_inputs)


def solution(mesh):
    in_specs = (
        P(("section", "dp"), None),
        P(("section", "dp")),
        P(("section", "dp")),
        P(None, None, "mp"),
        P("mp", None),
        P(),
        P(),
        P("mp", ("section", "dp")),
        P(("section", "dp")),
        P(("section", "dp"), "mp"),
        P("mp"),
        P(("section", "dp"), "mp"),
        P(("section", "dp"), "mp"),
        P("mp"),
    )
    out_specs = (P(("section", "dp"), "mp"), P(("section", "dp"), "mp"))
    return jax.shard_map(
        per_device, mesh=mesh, in_specs=in_specs, out_specs=out_specs, check_vma=False
    )
```
